128 devices in a mesh: rhs: 1, col: 64 (over z, y, x), row: 2 (over core).
Axes of the slice: x: 4, y: 4, z: 4, core: 2. Of those that a mesh axis runs over, the one named last changes fastest.
Arguments:
- volume: bfloat16 [128, 128, 128, 64], P('row', 'col', None, 'rhs')
- a_one: bfloat16 [128, 128], replicated
- b_one: bfloat16 [128, 128], replicated
- a_two: bfloat16 [128, 128], replicated
- b_two: bfloat16 [128, 128], replicated
- a_three: bfloat16 [128, 128], replicated
- b_three: bfloat16 [128, 128], replicated
- spectrum: float32 [128, 128, 128], P('row', 'col')
Outputs:
- output: float32 [128, 128, 128, 64], P('row', 'col', None, 'rhs')
All inputs are finite; a program needn't handle non-finite values.
Results may differ from the reference program's by a relative error of at most 0.0126449.
Values are sent between devices in bfloat16 or wider.
A program may use at most 1 GiB of HBM per device.

```python
import jax
import jax.numpy as jnp

N1 = 128
N2 = 128
N3 = 128
C = 64


def orthonormal(rng_key, order_n):
    q_mat = jnp.linalg.qr(jax.random.normal(rng_key, (order_n, order_n), jnp.float32))[0]
    return q_mat.astype(jnp.bfloat16)


def setup_inputs(seed: int = 0, part: int = 0) -> dict:
    shared = jax.random.split(jax.random.key(seed), 7)
    vol_key = jax.random.fold_in(jax.random.key(seed + 1), part)
    volume = jax.random.normal(vol_key, (N1, N2, N3, C), jnp.float32).astype(jnp.bfloat16)
    spectrum = jnp.exp(jax.random.uniform(shared[6], (N1, N2, N3), jnp.float32, -1.15, 1.15))
    return {'volume': volume, 'a_one': orthonormal(shared[0], N1), 'b_one': orthonormal(shared[1], N1), 'a_two': orthonormal(shared[2], N2), 'b_two': orthonormal(shared[3], N2), 'a_three': orthonormal(shared[4], N3), 'b_three': orthonormal(shared[5], N3), 'spectrum': spectrum}


def mode_product(factor, tensor, form):
    return jnp.einsum(form, factor.astype(jnp.float32), tensor.astype(jnp.float32))


def reference(volume, a_one, b_one, a_two, b_two, a_three, b_three, spectrum):
    u_three = mode_product(a_three, volume, 'ka,ijar->ijkr').astype(jnp.bfloat16)
    u_one = mode_product(a_one, u_three, 'ia,ajkr->ijkr').astype(jnp.bfloat16)
    u_two = mode_product(a_two, u_one, 'ja,iakr->ijkr').astype(jnp.bfloat16)
    scaled = (spectrum[:, :, :, None] * u_two.astype(jnp.float32)).astype(jnp.bfloat16)
    v_two = mode_product(b_two, scaled, 'ja,iakr->ijkr').astype(jnp.bfloat16)
    v_one = mode_product(b_one, v_two, 'ia,ajkr->ijkr').astype(jnp.bfloat16)
    return mode_product(b_three, v_one, 'ka,ijar->ijkr')
```

```python
import functools

import jax
import jax.numpy as jnp
from jax import lax
from jax.experimental import pallas as pl
from jax.experimental.pallas import tpu as pltpu
from jax.sharding import PartitionSpec as P

MESH = pl.DeviceIdType.MESH
BF = jnp.bfloat16
F32 = jnp.float32
N = 128
C = 64
NCH = 4
R = C // NCH
HALF = N // 2
STEP = 37


def partner_at(t, col, row):
    off = lax.rem(t * STEP, N)
    row2 = lax.rem(row + off, 2)
    x = lax.rem(lax.rem(col, 4) + off // 2, 4)
    y = lax.rem(lax.rem(col // 4, 4) + off // 8, 4)
    z = lax.rem(col // 16 + off // 32, 4)
    return z * 16 + y * 4 + x, row2


def by_rows(factor, stack):
    for r in range(0, stack.shape[0], 2):
        pair = jnp.concatenate([stack[r], stack[r + 1]], axis=1)
        yield jnp.dot(factor, pair, preferred_element_type=F32)


def restack(products):
    parts = []
    for p in products:
        parts += [p[:, :N], p[:, N:]]
    return jnp.swapaxes(jnp.stack(parts, axis=0), 0, 1)


def exchange_kernel(x_ref, a1_ref, b1_ref, a2_ref, b2_ref, a3_ref, d_ref, v_ref,
                    xv, us, uu, m1, r1, m2, r2, vs, dv,
                    xsem, us_s, us_r, d_s, d_r, s1, q1, s2, q2, v_s, v_r, o_s):
    col, row = lax.axis_index("col"), lax.axis_index("row")
    me = col * 2 + row

    loads = []
    for k in range(2):
        j = (1 - row) if k == 0 else row
        load = pltpu.make_async_copy(x_ref.at[:, pl.ds(j, 1)], xv.at[:, pl.ds(k, 1)], xsem.at[k])
        load.start()
        loads.append(load)

    barrier = pltpu.get_barrier_semaphore()

    def greet(t, carry):
        c2, g2 = partner_at(t, col, row)
        pl.semaphore_signal(barrier, inc=1, device_id=(0, c2, g2), device_id_type=MESH)
        return carry

    lax.fori_loop(1, N, greet, 0)

    def mode_three(k, block, out):
        rows = xv[pl.ds(block * 16, 16), k].reshape(16 * C, N)
        u = lax.dot_general(rows, a3_ref[...], (((1,), (1,)), ((), ())), preferred_element_type=F32)
        out[pl.ds(block * 16 + (0 if k == 0 else row * HALF), 16)] = u.astype(BF).reshape(16, C, N)

    loads[0].wait()

    def three_a(b, carry):
        mode_three(0, b, us)
        return carry

    lax.fori_loop(0, 4, three_a, 0)
    loads[1].wait()

    def three_b(b, carry):
        mode_three(1, b, uu)
        return carry

    lax.fori_loop(0, 4, three_b, 0)

    pl.semaphore_wait(barrier, N - 1)

    def swap_u(ch):
        part = pl.ds(pl.multiple_of(ch * R, R), R)
        return pltpu.make_async_remote_copy(
            src_ref=us.at[:, part], dst_ref=uu.at[pl.ds(row * HALF, HALF), part],
            send_sem=us_s.at[ch], recv_sem=us_r.at[ch],
            device_id=(0, col, 1 - row), device_id_type=MESH)

    for ch in range(NCH):
        swap_u(ch).start()

    def send_d(t, carry):
        i = lax.rem(t * STEP, HALF)
        target = row * HALF + i

        @pl.when(target != me)
        def _():
            pltpu.make_async_remote_copy(
                src_ref=d_ref.at[i], dst_ref=dv.at[col], send_sem=d_s, recv_sem=d_r,
                device_id=(0, target // 2, lax.rem(target, 2)), device_id_type=MESH).start()

        @pl.when(target == me)
        def _():
            dv[col] = d_ref[i]

        return carry

    lax.fori_loop(0, HALF, send_d, 0)

    def fan_out(ch, src, dst, ssem, rsem):
        def body(t, carry):
            c2, g2 = partner_at(t, col, row)
            pltpu.make_async_remote_copy(
                src_ref=src.at[ch, c2 * 2 + g2], dst_ref=dst.at[ch, me],
                send_sem=ssem.at[ch], recv_sem=rsem.at[ch],
                device_id=(0, c2, g2), device_id_type=MESH).start()
            return carry

        lax.fori_loop(1, N, body, 0)
        dst[ch, me] = src[ch, me]

    def wait_all(buf, ch, sem):
        whole = buf.at[ch, pl.ds(0, N - 1)]
        pltpu.make_async_copy(whole, whole, sem.at[ch]).wait()

    def first(ch, carry):
        swap_u(ch).wait_recv()
        part = pl.ds(pl.multiple_of(ch * R, R), R)
        stack = jnp.swapaxes(uu[:, part], 0, 1)
        m1[ch] = restack(p.astype(BF) for p in by_rows(a1_ref[...], stack))
        fan_out(ch, m1, r1, s1, q1)
        return carry

    lax.fori_loop(0, NCH, first, 0)

    mine = row == col // (HALF // 2)

    @pl.when(mine)
    def _():
        part = dv.at[pl.ds(0, HALF - 1)]
        pltpu.make_async_copy(part, part, d_r).wait()

    @pl.when(jnp.logical_not(mine))
    def _():
        pltpu.make_async_copy(dv, dv, d_r).wait()

    def second(ch, carry):
        wait_all(r1, ch, q1)
        diag = dv[...].reshape(N, N)
        diag = jnp.concatenate([diag, diag], axis=1)
        stack = jnp.swapaxes(r1[ch], 0, 1)
        outs = []
        for p in by_rows(a2_ref[...], stack):
            w = (diag * p.astype(BF).astype(F32)).astype(BF)
            outs.append(jnp.dot(b2_ref[...], w, preferred_element_type=F32).astype(BF))
        m2[ch] = restack(outs)
        fan_out(ch, m2, r2, s2, q2)
        return carry

    lax.fori_loop(0, NCH, second, 0)

    def swap_v(ch):
        part = pl.ds(pl.multiple_of(ch * R, R), R)
        return pltpu.make_async_remote_copy(
            src_ref=vs.at[pl.ds((1 - row) * HALF, HALF), part], dst_ref=v_ref.at[row, :, part],
            send_sem=v_s.at[ch], recv_sem=v_r.at[ch],
            device_id=(0, col, 1 - row), device_id_type=MESH)

    def keep_v(ch):
        part = pl.ds(pl.multiple_of(ch * R, R), R)
        return pltpu.make_async_copy(
            vs.at[pl.ds(row * HALF, HALF), part], v_ref.at[row, :, part], o_s.at[ch])

    def third(ch, carry):
        wait_all(r2, ch, q2)
        part = pl.ds(pl.multiple_of(ch * R, R), R)
        stack = jnp.swapaxes(r2[ch], 0, 1)
        vs[:, part] = restack(p.astype(BF) for p in by_rows(b1_ref[...], stack))
        swap_v(ch).start()
        keep_v(ch).start()
        return carry

    lax.fori_loop(0, NCH, third, 0)

    @pl.when(mine)
    def _():
        part = dv.at[pl.ds(0, HALF - 1)]
        pltpu.make_async_copy(part, part, d_s).wait()

    @pl.when(jnp.logical_not(mine))
    def _():
        pltpu.make_async_copy(dv, dv, d_s).wait()

    def drain(ch, carry):
        swap_u(ch).wait_send()
        wait_all(m1, ch, s1)
        wait_all(m2, ch, s2)
        swap_v(ch).wait()
        keep_v(ch).wait()
        return carry

    lax.fori_loop(0, NCH, drain, 0)


def exchange(x, a1, b1, a2, b2, a3, d):
    dma = pltpu.SemaphoreType.DMA
    vmem = pl.BlockSpec(memory_space=pltpu.VMEM)
    hbm = pl.BlockSpec(memory_space=pl.ANY)
    return pl.pallas_call(
        exchange_kernel,
        out_shape=jax.ShapeDtypeStruct((2, HALF, C, N), BF),
        in_specs=[hbm] + [vmem] * 6,
        out_specs=hbm,
        scratch_shapes=[
            pltpu.VMEM((HALF, 2, C, N), BF),
            pltpu.VMEM((HALF, C, N), BF),
            pltpu.VMEM((N, C, N), BF),
            pltpu.VMEM((NCH, N, R, N), BF),
            pltpu.VMEM((NCH, N, R, N), BF),
            pltpu.VMEM((NCH, N, R, N), BF),
            pltpu.VMEM((NCH, N, R, N), BF),
            pltpu.VMEM((N, C, N), BF),
            pltpu.VMEM((HALF, 2, N), F32),
            dma((2,)), dma((NCH,)), dma((NCH,)), dma, dma,
            dma((NCH,)), dma((NCH,)), dma((NCH,)), dma((NCH,)),
            dma((NCH,)), dma((NCH,)), dma((NCH,)),
        ],
        compiler_params=pltpu.CompilerParams(
            collective_id=0, has_side_effects=True, vmem_limit_bytes=40 << 20),
        name="exchange",
    )(x, a1, b1, a2, b2, a3, d)


def last_kernel(v_ref, b3_ref, z_ref):
    for j in range(2):
        rows = v_ref[j].reshape(-1, N)
        z = lax.dot_general(rows, b3_ref[...], (((1,), (1,)), ((), ())), preferred_element_type=F32)
        z_ref[:, j] = z.reshape(z_ref.shape[0], C, N)


def last(v, b3):
    step = 8
    return pl.pallas_call(
        last_kernel,
        grid=(HALF // step,),
        out_shape=jax.ShapeDtypeStruct((HALF, 2, C, N), F32),
        in_specs=[pl.BlockSpec((2, step, C, N), lambda i: (0, i, 0, 0)),
                  pl.BlockSpec((N, N), lambda i: (0, 0))],
        out_specs=pl.BlockSpec((step, 2, C, N), lambda i: (i, 0, 0, 0)),
        name="last",
    )(v, b3)


def solution(mesh):
    vol_spec = P("row", "col", None, "rhs")
    diag_spec = P("row", "col", None)
    full = P(None, None)

    def local_op(volume, a_one, b_one, a_two, b_two, a_three, b_three, spectrum):
        x = jnp.swapaxes(volume, 2, 3)
        v = exchange(x, a_one, b_one, a_two, b_two, a_three, spectrum)
        return jnp.swapaxes(last(v, b_three), 2, 3)

    return jax.shard_map(local_op, mesh=mesh, in_specs=(vol_spec,) + (full,) * 6 + (diag_spec,),
                         out_specs=vol_spec, check_vma=False)
```

```python
import functools

import jax
import jax.numpy as jnp
from jax import lax
from jax.experimental import pallas as pl
from jax.experimental.pallas import tpu as pltpu
from jax.sharding import PartitionSpec as P

MESH, LOGICAL = pl.DeviceIdType.MESH, pl.DeviceIdType.LOGICAL
BF = jnp.bfloat16
F32 = jnp.float32
N = 128
C = 64
NCH = 4
R = C // NCH
HALF = N // 2


def each_partner(me, act):
    def body(t, carry):
        base = lax.bitwise_xor(me, t * 8)
        for u in range(8):
            peer = lax.bitwise_xor(base, ((5 * u) % 16) * 8 + u)
            if u == 0:
                pl.when(t > 0)(functools.partial(act, peer))
            else:
                act(peer)
        return carry

    lax.fori_loop(0, 16, body, 0)


def by_rows(factor, stack):
    for r in range(0, stack.shape[0], 2):
        pair = jnp.concatenate([stack[r], stack[r + 1]], axis=1)
        yield jnp.dot(factor, pair, preferred_element_type=F32)


def restack(products):
    parts = []
    for p in products:
        parts += [p[:, :N], p[:, N:]]
    return jnp.swapaxes(jnp.stack(parts, axis=0), 0, 1)


def exchange_kernel(x_ref, a1_hbm, b1_hbm, a2_hbm, b2_hbm, a3_hbm, d_hbm, v_ref,
                    xv, us, uu, m1, r1, m2, r2, vs, dv,
                    a1_ref, b1_ref, a2_ref, b2_ref, a3_ref, d_ref,
                    xsem, fsem, us_s, us_r, d_s, d_r, s1, q1, s2, q2, v_s, v_r):
    col, row = lax.axis_index("col"), lax.axis_index("row")
    me = col * 2 + row
    other = 1 - row
    mine = row == col // (HALF // 2)

    loads = [pltpu.make_async_copy(a3_hbm, a3_ref, fsem.at[0])]
    for k in range(2):
        j = other if k == 0 else row
        loads.append(pltpu.make_async_copy(x_ref.at[:, pl.ds(j, 1)], xv.at[:, pl.ds(k, 1)], xsem.at[k]))
    loads += [
        pltpu.make_async_copy(a1_hbm, a1_ref, fsem.at[1]),
        pltpu.make_async_copy(d_hbm, d_ref, fsem.at[2]),
        pltpu.make_async_copy(a2_hbm, a2_ref, fsem.at[3]),
        pltpu.make_async_copy(b2_hbm, b2_ref, fsem.at[4]),
        pltpu.make_async_copy(b1_hbm.at[pl.ds(row * HALF, HALF)], b1_ref.at[pl.ds(0, HALF)], fsem.at[5]),
        pltpu.make_async_copy(b1_hbm.at[pl.ds(other * HALF, HALF)], b1_ref.at[pl.ds(HALF, HALF)], fsem.at[6]),
    ]
    for load in loads:
        load.start()

    barrier = pltpu.get_barrier_semaphore()

    def greet(peer):
        pl.semaphore_signal(barrier, inc=1, device_id=peer, device_id_type=LOGICAL)

    each_partner(me, greet)

    def mode_three(k, block, out):
        rows = xv[pl.ds(block * 16, 16), k].reshape(16 * C, N)
        u = lax.dot_general(rows, a3_ref[...], (((1,), (1,)), ((), ())), preferred_element_type=F32)
        out[pl.ds(block * 16 + (0 if k == 0 else row * HALF), 16)] = u.astype(BF).reshape(16, C, N)

    loads[0].wait()
    loads[1].wait()

    def three_a(b, carry):
        mode_three(0, b, us)
        return carry

    lax.fori_loop(0, 4, three_a, 0)
    loads[2].wait()

    def three_b(b, carry):
        mode_three(1, b, uu)
        return carry

    lax.fori_loop(0, 4, three_b, 0)
    for load in loads[3:]:
        load.wait()

    pl.semaphore_wait(barrier, N - 1)

    def swap_u(ch):
        part = pl.ds(pl.multiple_of(ch * R, R), R)
        return pltpu.make_async_remote_copy(
            src_ref=us.at[:, part], dst_ref=uu.at[pl.ds(row * HALF, HALF), part],
            send_sem=us_s.at[ch], recv_sem=us_r.at[ch],
            device_id=(0, col, other), device_id_type=MESH)

    for ch in range(NCH):
        swap_u(ch).start()

    low = lax.rem(me, HALF)

    def give_d(i):
        pltpu.make_async_remote_copy(
            src_ref=d_ref.at[i], dst_ref=dv.at[col], send_sem=d_s, recv_sem=d_r,
            device_id=row * HALF + i, device_id_type=LOGICAL).start()

    def send_d(t, carry):
        base = lax.bitwise_xor(low, t * 8)
        for u in range(8):
            i = lax.bitwise_xor(base, u)
            if u == 0:
                pl.when(jnp.logical_or(t > 0, jnp.logical_not(mine)))(functools.partial(give_d, i))
            else:
                give_d(i)
        return carry

    @pl.when(mine)
    def _():
        dv[col] = d_ref[low]

    lax.fori_loop(0, 8, send_d, 0)

    def fan_out(ch, src, dst, ssem, rsem):
        def send(peer):
            pltpu.make_async_remote_copy(
                src_ref=src.at[ch, peer], dst_ref=dst.at[ch, me],
                send_sem=ssem.at[ch], recv_sem=rsem.at[ch],
                device_id=peer, device_id_type=LOGICAL).start()

        each_partner(me, send)
        dst[ch, me] = src[ch, me]

    def wait_all(buf, ch, sem):
        whole = buf.at[ch, pl.ds(0, N - 1)]
        pltpu.make_async_copy(whole, whole, sem.at[ch]).wait()

    def first(ch, carry):
        swap_u(ch).wait_recv()
        part = pl.ds(pl.multiple_of(ch * R, R), R)
        stack = jnp.swapaxes(uu[:, part], 0, 1)
        m1[ch] = restack(p.astype(BF) for p in by_rows(a1_ref[...], stack))
        fan_out(ch, m1, r1, s1, q1)
        return carry

    lax.fori_loop(0, NCH, first, 0)

    @pl.when(mine)
    def _():
        part = dv.at[pl.ds(0, HALF - 1)]
        pltpu.make_async_copy(part, part, d_r).wait()

    @pl.when(jnp.logical_not(mine))
    def _():
        pltpu.make_async_copy(dv, dv, d_r).wait()

    def second(ch, carry):
        wait_all(r1, ch, q1)
        diag = dv[...].reshape(N, N)
        diag = jnp.concatenate([diag, diag], axis=1)
        stack = jnp.swapaxes(r1[ch], 0, 1)
        outs = []
        for p in by_rows(a2_ref[...], stack):
            w = (diag * p.astype(BF).astype(F32)).astype(BF)
            outs.append(jnp.dot(b2_ref[...], w, preferred_element_type=F32).astype(BF))
        m2[ch] = restack(outs)
        fan_out(ch, m2, r2, s2, q2)
        return carry

    lax.fori_loop(0, NCH, second, 0)

    def swap_v(ch):
        part = pl.ds(pl.multiple_of(ch * R, R), R)
        return pltpu.make_async_remote_copy(
            src_ref=vs.at[:, part], dst_ref=v_ref.at[row, :, part],
            send_sem=v_s.at[ch], recv_sem=v_r.at[ch],
            device_id=(0, col, other), device_id_type=MESH)

    def third(ch, carry):
        wait_all(r2, ch, q2)
        part = pl.ds(pl.multiple_of(ch * R, R), R)
        stack = jnp.swapaxes(r2[ch], 0, 1)
        v = restack(p.astype(BF) for p in by_rows(b1_ref[...], stack))
        vs[:, part] = v[HALF:]
        swap_v(ch).start()
        v_ref[row, :, part] = v[:HALF]
        return carry

    lax.fori_loop(0, NCH, third, 0)

    @pl.when(mine)
    def _():
        part = dv.at[pl.ds(0, HALF - 1)]
        pltpu.make_async_copy(part, part, d_s).wait()

    @pl.when(jnp.logical_not(mine))
    def _():
        pltpu.make_async_copy(dv, dv, d_s).wait()

    def drain(ch, carry):
        swap_u(ch).wait_send()
        wait_all(m1, ch, s1)
        wait_all(m2, ch, s2)
        swap_v(ch).wait()
        return carry

    lax.fori_loop(0, NCH, drain, 0)


def exchange(x, a1, b1, a2, b2, a3, d):
    dma = pltpu.SemaphoreType.DMA
    hbm = pl.BlockSpec(memory_space=pltpu.HBM)
    return pl.pallas_call(
        exchange_kernel,
        out_shape=jax.ShapeDtypeStruct((2, HALF, C, N), BF),
        in_specs=[hbm] * 7,
        out_specs=pl.BlockSpec(memory_space=pltpu.VMEM),
        scratch_shapes=[
            pltpu.VMEM((HALF, 2, C, N), BF),
            pltpu.VMEM((HALF, C, N), BF),
            pltpu.VMEM((N, C, N), BF),
            pltpu.VMEM((NCH, N, R, N), BF),
            pltpu.VMEM((NCH, N, R, N), BF),
            pltpu.VMEM((NCH, N, R, N), BF),
            pltpu.VMEM((NCH, N, R, N), BF),
            pltpu.VMEM((HALF, C, N), BF),
            pltpu.VMEM((HALF, 2, N), F32),
            *[pltpu.VMEM((N, N), BF)] * 5,
            pltpu.VMEM((HALF, 2, N), F32),
            dma((2,)), dma((7,)), dma((NCH,)), dma((NCH,)), dma, dma,
            dma((NCH,)), dma((NCH,)), dma((NCH,)), dma((NCH,)),
            dma((NCH,)), dma((NCH,)),
        ],
        compiler_params=pltpu.CompilerParams(
            collective_id=0, has_side_effects=True, vmem_limit_bytes=40 << 20),
        name="exchange",
    )(*[pltpu.with_memory_space_constraint(v, pltpu.HBM) for v in (x, a1, b1, a2, b2, a3, d)])


def last_kernel(v_ref, b3_ref, z_ref, zv, zsem):
    step = 8

    def out(b):
        part = pl.ds(b * step, step)
        return pltpu.make_async_copy(zv.at[part], z_ref.at[part], zsem)

    def body(b, carry):
        for j in range(2):
            rows = v_ref[j, pl.ds(b * step, step)].reshape(step * C, N)
            z = lax.dot_general(rows, b3_ref[...], (((1,), (1,)), ((), ())), preferred_element_type=F32)
            zv[pl.ds(b * step, step), j] = z.reshape(step, C, N)
        out(b).start()
        return carry

    lax.fori_loop(0, HALF // step, body, 0)
    pltpu.make_async_copy(zv, z_ref, zsem).wait()


def last(v, b3):
    vmem = pl.BlockSpec(memory_space=pltpu.VMEM)
    return pl.pallas_call(
        last_kernel,
        out_shape=jax.ShapeDtypeStruct((HALF, 2, C, N), F32),
        in_specs=[vmem, vmem],
        out_specs=pl.BlockSpec(memory_space=pltpu.HBM),
        scratch_shapes=[pltpu.VMEM((HALF, 2, C, N), F32), pltpu.SemaphoreType.DMA],
        compiler_params=pltpu.CompilerParams(vmem_limit_bytes=16 << 20),
        name="last",
    )(v, b3)


def solution(mesh):
    vol_spec = P("row", "col", None, "rhs")
    diag_spec = P("row", "col", None)
    full = P(None, None)

    def local_op(volume, a_one, b_one, a_two, b_two, a_three, b_three, spectrum):
        x = jnp.swapaxes(volume, 2, 3)
        v = exchange(x, a_one, b_one, a_two, b_two, a_three, spectrum)
        return jnp.swapaxes(last(v, b_three), 2, 3)

    return jax.shard_map(local_op, mesh=mesh, in_specs=(vol_spec,) + (full,) * 6 + (diag_spec,),
                         out_specs=vol_spec, check_vma=False)
```
